512 devices in a mesh: tile: 16 (over y, x), depth: 32 (over z, core).
Axes of the slice: x: 4, y: 4, z: 16, core: 2. Of those that a mesh axis runs over, the one named last changes fastest.
Arguments:
- patches: float32 [1024, 256, 256], P('tile', 'depth'), may hold values from -6 to 6
- patch_owner: int32 [1024, 1], P('tile'), may hold values from 0 to 15; in each aligned block of 64 rows (0 to 63, 64 to 127, ...) at most 8 rows name the same one
- patch_level: int32 [1024], P('tile'), may hold values from 0 to 63
- phases: float32 [1024, 256, 256], P('tile', None, 'depth'), may hold values from -3.140625 to 3.140625
Outputs:
- intensity: float32 [1024, 256, 256], P('tile', 'depth')
The draws below stay inside these ranges and needn't reach their ends.
Inputs may be any that keep to these rules, and one draw needn't show every extreme that they name: `patch_owner`: among the 64 patches of one index of tile, at most 8 have the same owner.
All inputs are finite; a program needn't handle non-finite values.
Results may differ from the reference program's by a relative error of at most 0.00017.
Values sent between devices are 32-bit elements; how exact they have to be, the bound alone decides.
A program may use at most 64 MiB of HBM per device.

```python
import math
import jax
import jax.numpy as jnp
import numpy as np
from jax import lax

M = 256
P_DEV = 64
CAP = 8
DEP_DEV = 64
OWNERS = 16
DEPTHS = 1024
PATCHES = 1024


def set_ends(values, rng, smallest, high):
    longest = values.shape.index(max(values.shape))
    spots = []
    for shift in (0, 1):
        where = [jax.random.randint(jax.random.fold_in(rng, axis), (), 0, length) for axis, length in enumerate(values.shape)]
        where[longest] = (where[longest] + shift) % values.shape[longest]
        spots.append(tuple(where))
    return values.at[spots[0]].set(smallest).at[spots[1]].set(high)


def levels(rng, dims, split, smallest, largest):
    level, own = 1.0, jax.random.fold_in(rng, 6)
    for axis_at, shards_of in split:
        heights = jnp.exp(jax.random.uniform(jax.random.fold_in(own, axis_at), (shards_of,), jnp.float32, smallest / len(split), largest / len(split)))
        level = level * jnp.repeat(heights, dims[axis_at] // shards_of).reshape([-1 if axis == axis_at else 1 for axis in range(len(dims))])
    return level


def routed_block(stream_key, own, number, rows, number_of, top, limit, slope):
    ranking = jax.random.permutation(stream_key, number_of)
    packed, common = portions_of(number_of, rows * top, limit, slope, True), portions_of(number_of, rows * top, limit, slope, False)
    places = jnp.arange(number_of)

    def named(lengths, turn):
        used = int((lengths > 0).sum())
        fixed = max(1, used // 4)
        shifted = fixed + (places - fixed + turn * (used - fixed)) % max(1, number_of - fixed)
        return jnp.zeros((number_of,), jnp.int32).at[ranking[jnp.where(places < fixed, places, shifted)]].set(jnp.asarray(lengths, jnp.int32))

    lengths = jnp.where(number % 4 == 0, named(packed, number // 4), named(common, number - number // 4 - 1))
    mixed = jax.random.permutation(jax.random.fold_in(own, 3), number_of)
    donor, taker = mixed[0:number_of // 2 * 2:2], mixed[1:number_of // 2 * 2:2]
    margin = jnp.minimum(lengths[donor] - 1, limit - lengths[taker]) // 2
    margin = jnp.where((donor == ranking[0]) | (taker == ranking[0]) | (lengths[taker] == 0), 0, jnp.maximum(margin, 0))
    shifted = jax.random.randint(jax.random.fold_in(own, 4), (number_of // 2,), 0, 1 << 20) % (margin + 1)
    lengths = lengths.at[donor].add(-shifted).at[taker].add(shifted)
    members = jnp.searchsorted(jnp.cumsum(lengths), jnp.arange(rows * top), side="right").astype(jnp.int32)
    listing = members.reshape(top, rows).T
    listing = listing[jax.random.permutation(jax.random.fold_in(own, 1), rows)]
    turn = jax.random.randint(jax.random.fold_in(own, 2), (rows, 1), 0, top)
    return jnp.take_along_axis(listing, (jnp.arange(top)[None, :] + turn) % top, axis=1)


def portions_of(amount, total, most, lean, full):
    weights = [(1 << 20) // math.isqrt(grade ** lean) + 1 for grade in range(1, amount + 1)]
    largest = most if full else min(most, max(-(-total // amount), total * weights[0] // sum(weights)))
    least = 1 if total - largest >= amount - 1 else 0
    counts, spare = [largest] + [least] * (amount - 1), total - largest - least * (amount - 1)
    while spare > 0:
        movable = [i for i in range(1, amount) if counts[i] < largest] or [i for i in range(1, amount) if counts[i] < most]
        mass, remaining = sum([weights[i] for i in movable]), spare
        for i in movable:
            more = min(most - counts[i], max(1, remaining * weights[i] // mass), spare)
            counts[i] = counts[i] + more
            spare = spare - more
    return np.array(counts)


def centred(key, shape, width, most, cuts=(), dtype=jnp.bfloat16):
    loudness = levels(key, shape, cuts, -0.22, 0.18) if cuts else 1.0
    entries = jax.random.normal(key, shape, jnp.float32) * width * loudness
    return jnp.minimum(jnp.maximum(entries, -most), most).astype(dtype)


def setup_inputs(seed: int = 0) -> dict:
    arg_keys = jax.random.split(jax.random.key(seed), 5)
    patches = centred(arg_keys[0], (PATCHES, M, M), 1.0, 6.0, ((0, 16), (1, 32)), jnp.float32)
    patch_owner_keys = jax.random.split(jax.random.fold_in(arg_keys[1], 1), PATCHES // P_DEV)
    patch_owner_turns = jax.random.permutation(jax.random.fold_in(arg_keys[1], 3), PATCHES // P_DEV)
    patch_owner = jax.vmap(lambda own, number: routed_block(jax.random.fold_in(arg_keys[1], 2), own, number, P_DEV, OWNERS, 1, CAP, 2))(patch_owner_keys, patch_owner_turns).reshape((PATCHES, 1))
    patch_level = set_ends(jax.random.randint(arg_keys[2], (PATCHES,), 0, DEP_DEV), jax.random.fold_in(arg_keys[2], 1), 0, DEP_DEV - 1).astype(jnp.int32)
    phases = jnp.clip(jax.random.uniform(arg_keys[3], (DEPTHS, M, M), jnp.float32, -3.140625, 3.140625), -3.140625, 3.140625)
    return dict(patches=patches, patch_owner=patch_owner, patch_level=patch_level, phases=phases)


def reference(patches, patch_owner, patch_level, phases):
    depth_index = (patch_owner[:, 0] * DEP_DEV + patch_level).astype(jnp.int32)

    def propagate(items):
        patch, chosen = items
        phase = phases[chosen]
        spectrum = jnp.fft.fft2(patch)
        field = jnp.fft.ifft2(spectrum * (jnp.cos(phase) + 1j * jnp.sin(phase)))
        return jnp.real(field) ** 2 + jnp.imag(field) ** 2

    return lax.map(propagate, (patches, depth_index))
```

```python
import functools
import math

import jax
import jax.numpy as jnp
import numpy as np
from jax import lax
from jax.experimental import pallas as pl
from jax.experimental.pallas import tpu as pltpu
from jax.sharding import PartitionSpec as P

CAP = 8
LANES = 128


def dft_tables(extent):
    indices = np.arange(extent)
    angles = (indices[:, None] * indices[None, :] % extent) * (2.0 * math.pi / extent)
    exact = np.concatenate([np.cos(angles), np.sin(angles)], axis=0)
    high = exact.astype(np.float32).astype(jnp.bfloat16)
    low = (exact - high.astype(np.float64)).astype(np.float32).astype(jnp.bfloat16)
    return np.concatenate([high, low, high], axis=1)


def split(values):
    high = values.astype(jnp.bfloat16)
    low = (values - high.astype(jnp.float32)).astype(jnp.bfloat16)
    return high, low


def apply_left(table, values):
    high, low = split(values)
    stacked = jnp.concatenate([high, high, low], axis=0)
    return jnp.dot(table, stacked, preferred_element_type=jnp.float32)


def apply_left_transposed(table, values):
    high, low = split(values)
    stacked = jnp.concatenate([high, high, low], axis=1)
    return lax.dot_general(table, stacked, (((1,), (1,)), ((), ())), preferred_element_type=jnp.float32)


def polynomial(square, terms):
    total = jnp.full_like(square, terms[-1])
    for term in terms[-2::-1]:
        total = total * square + term
    return total


SIN_TERMS = [(-1.0) ** n / math.factorial(2 * n + 1) for n in range(7)]
COS_TERMS = [(-1.0) ** n / math.factorial(2 * n) for n in range(8)]


def cos_sin(phase):
    half = phase * 0.5
    square = half * half
    sine = half * polynomial(square, SIN_TERMS)
    cosine = polynomial(square, COS_TERMS)
    return 1.0 - 2.0 * sine * sine, 2.0 * sine * cosine


def far_first(step, extent):
    return extent // 2 + (step // 2) * (1 - 2 * (step % 2)) - step % 2


def kernel(
    tiles,
    patches,
    owner,
    level,
    phases,
    tables,
    out,
    table,
    depths,
    slot_row,
    slot_at,
    want_row,
    wants,
    wants_at,
    packed,
    got,
    chosen,
    pixels,
    phase,
    spectrum,
    intensity,
    local_sem,
    want_send,
    want_recv,
    pack_send,
    pack_recv,
    pixel_send,
    pixel_recv,
    phase_send,
    phase_recv,
    out_send,
    out_recv,
):
    count, rows, extent = patches.shape
    spread = extent // rows
    ring = spread // 2
    own = count // spread
    side = math.isqrt(tiles)
    me_t, me_d = lax.axis_index("tile"), lax.axis_index("depth")
    me_y, me_x, me_z, me_c = me_t // side, me_t % side, me_d // 2, me_d % 2

    def depth_pair(step):
        hop, swap = far_first(step // 2, ring), 1 - step % 2
        to = ((me_z + hop) % ring) * 2 + (me_c + swap) % 2
        source = ((me_z + ring - hop) % ring) * 2 + (me_c + swap) % 2
        return to, source

    def tile_pair(step):
        down, over = far_first(step // side, side), far_first(step % side, side)
        to = ((me_y + down) % side) * side + (me_x + over) % side
        source = ((me_y + side - down) % side) * side + (me_x + side - over) % side
        return to, source

    depth_steps, tile_steps = spread - 1, tiles - 1

    barrier = pltpu.get_barrier_semaphore()

    @pl.loop(0, depth_steps)
    def _(step):
        pl.semaphore_signal(barrier, inc=1, device_id={"depth": depth_pair(step)[0]})

    @pl.loop(0, tile_steps)
    def _(step):
        pl.semaphore_signal(barrier, inc=1, device_id={"tile": tile_pair(step)[0]})

    load_depths = pltpu.make_async_copy(phases, depths, local_sem.at[0])
    load_depths.start()
    load_table = pltpu.make_async_copy(tables, table, local_sem.at[1])
    load_table.start()
    load_pixels = pltpu.make_async_copy(
        patches.at[pl.ds(me_d * own, own)], pixels.at[:, pl.ds(me_d * rows, rows), :], local_sem.at[2]
    )
    load_pixels.start()

    lane = lax.broadcasted_iota(jnp.int32, (1, LANES), 1)
    owners = lax.fori_loop(
        0, count, lambda p, row: jnp.where(lane == p, owner[0, p], row), jnp.full((1, LANES), -1, jnp.int32)
    )
    ranks = lax.fori_loop(
        0,
        count,
        lambda p, row: row + jnp.where((owners == owner[0, p]) & (lane > p), 1, 0),
        jnp.zeros((1, LANES), jnp.int32),
    )
    slot_row[...] = owners * CAP + ranks
    load_slots = pltpu.make_async_copy(slot_row, slot_at, local_sem.at[3])
    load_slots.start()
    load_slots.wait()
    wanted = lax.fori_loop(
        0,
        count,
        lambda p, row: jnp.where(lane == slot_at[0, p], level[0, p], row),
        jnp.zeros((1, LANES), jnp.int32),
    )
    want_row[...] = wanted
    wants[me_t] = wanted

    pl.semaphore_wait(barrier, depth_steps + tile_steps)

    def want_copy(step, to, source):
        return pltpu.make_async_remote_copy(
            src_ref=want_row,
            dst_ref=wants.at[source],
            send_sem=want_send.at[step],
            recv_sem=want_recv.at[step],
            device_id={"tile": to},
        )

    def pixel_copy(step, to, source):
        return pltpu.make_async_remote_copy(
            src_ref=patches.at[pl.ds(to * own, own)],
            dst_ref=pixels.at[:, pl.ds(source * rows, rows), :],
            send_sem=pixel_send.at[step],
            recv_sem=pixel_recv.at[step],
            device_id={"depth": to},
        )

    def pack_copy(step, to, source):
        return pltpu.make_async_remote_copy(
            src_ref=packed.at[to],
            dst_ref=got.at[pl.ds(source * CAP, CAP)],
            send_sem=pack_send.at[step],
            recv_sem=pack_recv.at[step],
            device_id={"tile": to},
        )

    def phase_copy(which, step, to, source):
        return pltpu.make_async_remote_copy(
            src_ref=chosen.at[which, to],
            dst_ref=phase.at[which, pl.ds(source * rows, rows), :],
            send_sem=phase_send.at[which, step],
            recv_sem=phase_recv.at[which, step],
            device_id={"depth": to},
        )

    def out_copy(which, step, to, source):
        return pltpu.make_async_remote_copy(
            src_ref=intensity.at[which, pl.ds(to * rows, rows), :],
            dst_ref=out.at[source * own + which],
            send_sem=out_send.at[which, step],
            recv_sem=out_recv.at[which, step],
            device_id={"depth": to},
        )

    @pl.loop(0, tile_steps)
    def _(step):
        want_copy(step, tile_pair(step)[0], me_t).start()

    @pl.loop(0, depth_steps)
    def _(step):
        pixel_copy(step, depth_pair(step)[0], me_d).start()

    load_depths.wait()

    @pl.loop(0, tile_steps)
    def _(step):
        to, source = tile_pair(step)
        want_copy(step, to, source).wait_recv()

    load_wants = pltpu.make_async_copy(wants, wants_at, local_sem.at[3])
    load_wants.start()
    load_wants.wait()

    @pl.loop(0, tile_steps)
    def _(step):
        to = tile_pair(step)[0]
        for slot in range(CAP):
            packed[to, slot] = depths[wants_at[to, 0, me_t * CAP + slot]]
        pack_copy(step, to, me_t).start()

    for slot in range(CAP):
        got[me_t * CAP + slot] = depths[wants_at[me_t, 0, me_t * CAP + slot]]

    @pl.loop(0, tile_steps)
    def _(step):
        to, source = tile_pair(step)
        pack_copy(step, to, source).wait_recv()

    @pl.loop(0, own)
    def _(which):
        @pl.loop(0, depth_steps)
        def _(step):
            to = depth_pair(step)[0]
            chosen[which, to] = got[slot_at[0, to * own + which]]
            phase_copy(which, step, to, me_d).start()

        phase[which, pl.ds(me_d * rows, rows), :] = got[slot_at[0, me_d * own + which]]

    load_table.wait()
    load_pixels.wait()

    @pl.loop(0, depth_steps)
    def _(step):
        to, source = depth_pair(step)
        pixel_copy(step, to, source).wait_recv()

    @pl.loop(0, own)
    def _(which):
        columns = apply_left(table[...], pixels[which])
        both = apply_left_transposed(table[...], columns)
        spectrum[which, 0] = both[:extent, :extent] - both[extent:, extent:]
        spectrum[which, 1] = -(both[:extent, extent:] + both[extent:, :extent])

    @pl.loop(0, own)
    def _(which):
        @pl.loop(0, depth_steps)
        def _(step):
            to, source = depth_pair(step)
            phase_copy(which, step, to, source).wait_recv()

        cosine, sine = cos_sin(phase[which])
        scale = 1.0 / float(extent * extent)
        real, imag = spectrum[which, 0] * scale, spectrum[which, 1] * scale
        moved = jnp.concatenate([real * cosine - imag * sine, real * sine + imag * cosine], axis=1)
        both = apply_left(table[...], moved)
        back = jnp.concatenate(
            [both[:extent, :extent] - both[extent:, extent:], both[:extent, extent:] + both[extent:, :extent]], axis=0
        )
        both = apply_left_transposed(table[...], back)
        field_real = both[:extent, :extent] - both[extent:, extent:]
        field_imag = both[:extent, extent:] + both[extent:, :extent]
        intensity[which] = field_real * field_real + field_imag * field_imag

        @pl.loop(0, depth_steps)
        def _(step):
            out_copy(which, step, depth_pair(step)[0], me_d).start()

        pltpu.make_async_copy(
            intensity.at[which, pl.ds(me_d * rows, rows), :], out.at[me_d * own + which], local_sem.at[4 + which]
        ).start()

    @pl.loop(0, tile_steps)
    def _(step):
        to, source = tile_pair(step)
        want_copy(step, to, source).wait_send()
        pack_copy(step, to, source).wait_send()

    @pl.loop(0, depth_steps)
    def _(step):
        to, source = depth_pair(step)
        pixel_copy(step, to, source).wait_send()

    @pl.loop(0, own)
    def _(which):
        @pl.loop(0, depth_steps)
        def _(step):
            to, source = depth_pair(step)
            phase_copy(which, step, to, source).wait_send()
            out_copy(which, step, to, source).wait()

        pltpu.make_async_copy(
            intensity.at[which, pl.ds(me_d * rows, rows), :], out.at[me_d * own + which], local_sem.at[4 + which]
        ).wait()


def solution(mesh):
    tiles, spread = mesh.shape["tile"], mesh.shape["depth"]

    def on_device(patches, patch_owner, patch_level, phases):
        count, rows, extent = patches.shape
        own = count // spread
        depth_count = phases.shape[0]
        tables = jnp.asarray(dft_tables(extent))
        any_space = pl.BlockSpec(memory_space=pl.ANY)
        scalars = pl.BlockSpec(memory_space=pltpu.SMEM)
        f32, dma = jnp.float32, pltpu.SemaphoreType.DMA
        return pl.pallas_call(
            functools.partial(kernel, tiles),
            out_shape=jax.ShapeDtypeStruct(patches.shape, patches.dtype),
            in_specs=[any_space, scalars, scalars, any_space, any_space],
            out_specs=any_space,
            scratch_shapes=[
                pltpu.VMEM(tables.shape, tables.dtype),
                pltpu.VMEM((depth_count, rows, extent), f32),
                pltpu.VMEM((1, LANES), jnp.int32),
                pltpu.SMEM((1, LANES), jnp.int32),
                pltpu.VMEM((1, LANES), jnp.int32),
                pltpu.VMEM((tiles, 1, LANES), jnp.int32),
                pltpu.SMEM((tiles, 1, LANES), jnp.int32),
                pltpu.VMEM((tiles, CAP, rows, extent), f32),
                pltpu.VMEM((tiles * CAP, rows, extent), f32),
                pltpu.VMEM((own, spread, rows, extent), f32),
                pltpu.VMEM((own, extent, extent), f32),
                pltpu.VMEM((own, extent, extent), f32),
                pltpu.VMEM((own, 2, extent, extent), f32),
                pltpu.VMEM((own, extent, extent), f32),
                dma((4 + own,)),
                dma((tiles,)),
                dma((tiles,)),
                dma((tiles,)),
                dma((tiles,)),
                dma((spread,)),
                dma((spread,)),
                dma((own, spread)),
                dma((own, spread)),
                dma((own, spread)),
                dma((own, spread)),
            ],
            compiler_params=pltpu.CompilerParams(
                collective_id=0, has_side_effects=True, vmem_limit_bytes=60 * 1024 * 1024
            ),
        )(
            patches,
            patch_owner.reshape(1, count),
            patch_level.reshape(1, count),
            jnp.transpose(phases, (0, 2, 1)),
            tables,
        )

    return jax.shard_map(
        on_device,
        mesh=mesh,
        in_specs=(P("tile", "depth", None), P("tile", None), P("tile"), P("tile", None, "depth")),
        out_specs=P("tile", "depth", None),
        check_vma=False,
    )
```

```python
import functools
import math

import jax
import jax.numpy as jnp
import numpy as np
from jax import lax
from jax.experimental import pallas as pl
from jax.experimental.pallas import tpu as pltpu
from jax.sharding import PartitionSpec as P

CAP = 8
LANES = 128
EDGES = (0, 1, 2, 3, 4, 8)


def dft_tables(extent):
    indices = np.arange(extent)
    angles = (indices[:, None] * indices[None, :] % extent) * (2.0 * math.pi / extent)
    exact = np.concatenate([np.cos(angles), np.sin(angles)], axis=0)
    high = exact.astype(np.float32).astype(jnp.bfloat16)
    low = (exact - high.astype(np.float64)).astype(np.float32).astype(jnp.bfloat16)
    return np.concatenate([high, low, high], axis=1)


def split(values):
    high = values.astype(jnp.bfloat16)
    low = (values - high.astype(jnp.float32)).astype(jnp.bfloat16)
    return high, low


def apply_left(table, values):
    high, low = split(values)
    stacked = jnp.concatenate([high, high, low], axis=0)
    return jnp.dot(table, stacked, preferred_element_type=jnp.float32)


def apply_left_transposed(table, values):
    high, low = split(values)
    stacked = jnp.concatenate([high, high, low], axis=1)
    return lax.dot_general(table, stacked, (((1,), (1,)), ((), ())), preferred_element_type=jnp.float32)


def polynomial(square, terms):
    total = jnp.full_like(square, terms[-1])
    for term in terms[-2::-1]:
        total = total * square + term
    return total


SIN_TERMS = [(-1.0) ** n / math.factorial(2 * n + 1) for n in range(7)]
COS_TERMS = [(-1.0) ** n / math.factorial(2 * n) for n in range(8)]


def cos_sin(phase):
    half = phase * 0.5
    square = half * half
    sine = half * polynomial(square, SIN_TERMS)
    cosine = polynomial(square, COS_TERMS)
    return 1.0 - 2.0 * sine * sine, 2.0 * sine * cosine


def near_first(step):
    return ((step + 1) // 2) * (2 * (step % 2) - 1)


def reaches(spread):
    half = spread // 4
    reach = max(1, half // 4)
    return reach, -(-(half - reach) // reach)


def kernel(
    tiles,
    patches,
    owner,
    level,
    phases,
    tables,
    out,
    table,
    depths,
    slot_row,
    slot_at,
    want_row,
    wants,
    wants_at,
    packed,
    got,
    chosen,
    pixels,
    phase,
    spectrum,
    intensity,
    ring_sem,
    local_sem,
    row_send,
    row_recv,
    want_send,
    want_recv,
    pack_send,
    pack_recv,
    pixel_send,
    pixel_recv,
    phase_send,
    phase_recv,
    out_send,
    out_recv,
):
    count, rows, extent = patches.shape
    spread = extent // rows
    ring = spread // 2
    own = count // spread
    side = math.isqrt(tiles)
    me_t, me_d = lax.axis_index("tile"), lax.axis_index("depth")
    me_y, me_x, me_z, me_c = me_t // side, me_t % side, me_d // 2, me_d % 2

    def peer(step):
        hop, swap = near_first(step // 2), step % 2
        to = ((me_z + ring + hop) % ring) * 2 + (me_c + swap) % 2
        source = ((me_z + ring - hop) % ring) * 2 + (me_c + swap) % 2
        return to, source

    def shifted(down, over):
        to = ((me_y + down) % side) * side + (me_x + over) % side
        source = ((me_y + side - down) % side) * side + (me_x + side - over) % side
        return to, source

    reach, ring_rounds = reaches(spread)

    def within(distance):
        return min(2 * (2 * distance + 1), spread)

    barrier = pltpu.get_barrier_semaphore()

    @pl.loop(1, within(reach))
    def _(step):
        pl.semaphore_signal(barrier, inc=1, device_id={"depth": peer(step)[0]})

    @pl.loop(1, side)
    def _(shift):
        pl.semaphore_signal(barrier, inc=1, device_id={"tile": shifted(0, shift)[0]})
        pl.semaphore_signal(barrier, inc=1, device_id={"tile": shifted(shift, 0)[0]})

    def tell_ring(turn):
        for way, hop in enumerate((reach, ring - reach)):
            to = ((me_z + hop) % ring) * 2 + me_c
            pl.semaphore_signal(ring_sem.at[turn, way], inc=1, device_id={"depth": to})

    def learn_ring(turn):
        for way in range(2):
            pl.semaphore_wait(ring_sem.at[turn, way], 1)
        if turn + 1 < ring_rounds:
            tell_ring(turn + 1)
        send_pixels(turn + 1)

    load_depths = pltpu.make_async_copy(phases, depths, local_sem.at[0])
    load_depths.start()
    load_table = pltpu.make_async_copy(tables, table, local_sem.at[1])
    load_table.start()
    load_pixels = pltpu.make_async_copy(
        patches.at[pl.ds(me_d * own, own)], pixels.at[:, pl.ds(me_d * rows, rows), :], local_sem.at[2]
    )
    load_pixels.start()

    lane = lax.broadcasted_iota(jnp.int32, (1, LANES), 1)
    owners = lax.fori_loop(
        0, count, lambda p, row: jnp.where(lane == p, owner[0, p], row), jnp.full((1, LANES), -1, jnp.int32)
    )
    ranks = lax.fori_loop(
        0,
        count,
        lambda p, row: row + jnp.where((owners == owner[0, p]) & (lane > p), 1, 0),
        jnp.zeros((1, LANES), jnp.int32),
    )
    slot_row[...] = owners * CAP + ranks
    load_slots = pltpu.make_async_copy(slot_row, slot_at, local_sem.at[3])
    load_slots.start()
    load_slots.wait()
    wanted = lax.fori_loop(
        0,
        count,
        lambda p, row: jnp.where(lane == slot_at[0, p], level[0, p], row),
        jnp.zeros((1, LANES), jnp.int32),
    )
    want_row[...] = wanted
    wants[me_t] = wanted

    pl.semaphore_wait(barrier, within(reach) - 1 + 2 * (side - 1))
    tell_ring(0)

    def row_copy(shift, source):
        return pltpu.make_async_remote_copy(
            src_ref=want_row,
            dst_ref=wants.at[source],
            send_sem=row_send.at[shift],
            recv_sem=row_recv.at[shift],
            device_id={"tile": shifted(0, shift)[0]},
        )

    def want_copy(shift, source_row):
        return pltpu.make_async_remote_copy(
            src_ref=wants.at[pl.ds(me_y * side, side)],
            dst_ref=wants.at[pl.ds(source_row * side, side)],
            send_sem=want_send.at[shift],
            recv_sem=want_recv.at[shift],
            device_id={"tile": shifted(shift, 0)[0]},
        )

    def pixel_copy(step, to, source):
        return pltpu.make_async_remote_copy(
            src_ref=patches.at[pl.ds(to * own, own)],
            dst_ref=pixels.at[:, pl.ds(source * rows, rows), :],
            send_sem=pixel_send.at[step],
            recv_sem=pixel_recv.at[step],
            device_id={"depth": to},
        )

    def pack_copy(step, to, source):
        return pltpu.make_async_remote_copy(
            src_ref=packed.at[to],
            dst_ref=got.at[pl.ds(source * CAP, CAP)],
            send_sem=pack_send.at[step],
            recv_sem=pack_recv.at[step],
            device_id={"tile": to},
        )

    def phase_copy(which, step, to, source):
        return pltpu.make_async_remote_copy(
            src_ref=chosen.at[which, to],
            dst_ref=phase.at[which, pl.ds(source * rows, rows), :],
            send_sem=phase_send.at[which, step],
            recv_sem=phase_recv.at[which, step],
            device_id={"depth": to},
        )

    def out_copy(which, step, to, source):
        return pltpu.make_async_remote_copy(
            src_ref=intensity.at[which, pl.ds(to * rows, rows), :],
            dst_ref=out.at[source * own + which],
            send_sem=out_send.at[which, step],
            recv_sem=out_recv.at[which, step],
            device_id={"depth": to},
        )

    def send_pixels(turn):
        first = 1 if turn == 0 else within(turn * reach)

        @pl.loop(first, within((turn + 1) * reach))
        def _(step):
            pixel_copy(step, peer(step)[0], me_d).start()

    def send_packed(down, over):
        to = shifted(down, over)[0]
        for slot in range(CAP):
            packed[to, slot] = depths[wants_at[to, 0, me_t * CAP + slot]]
        pack_copy(down * side + over, to, me_t).start()

    def read_wants(row):
        load = pltpu.make_async_copy(
            wants.at[pl.ds(row * side, side)], wants_at.at[pl.ds(row * side, side)], local_sem.at[3]
        )
        load.start()
        load.wait()

    @pl.loop(1, side)
    def _(shift):
        row_copy(shift, me_t).start()

    send_pixels(0)
    learn_ring(0)

    @pl.loop(1, side)
    def _(shift):
        row_copy(shift, shifted(0, shift)[1]).wait_recv()

    @pl.loop(1, side)
    def _(shift):
        want_copy(shift, me_y).start()

    for turn in range(1, ring_rounds):
        learn_ring(turn)
    load_depths.wait()
    read_wants(me_y)

    @pl.loop(1, side)
    def _(over):
        send_packed(0, over)

    @pl.loop(1, side)
    def _(turn):
        down = (side + near_first(turn)) % side
        want_copy(side - down, (me_y + down) % side).wait_recv()
        read_wants((me_y + down) % side)

        @pl.loop(0, side)
        def _(over):
            send_packed(down, over)

    for slot in range(CAP):
        got[me_t * CAP + slot] = depths[wants_at[me_t, 0, me_t * CAP + slot]]

    @pl.loop(1, tiles)
    def _(step):
        to, source = shifted(step // side, step % side)
        pack_copy(step, to, source).wait_recv()

    @pl.loop(0, own)
    def _(which):
        @pl.loop(1, spread)
        def _(turn):
            step = spread - turn
            to = peer(step)[0]
            chosen[which, to] = got[slot_at[0, to * own + which]]
            phase_copy(which, step, to, me_d).start()

        phase[which, pl.ds(me_d * rows, rows), :] = got[slot_at[0, me_d * own + which]]

    load_table.wait()
    load_pixels.wait()

    @pl.loop(1, spread)
    def _(step):
        to, source = peer(step)
        pixel_copy(step, to, source).wait_recv()

    @pl.loop(0, own)
    def _(which):
        columns = apply_left(table[...], pixels[which])
        both = apply_left_transposed(table[...], columns)
        spectrum[which, 0] = both[:extent, :extent] - both[extent:, extent:]
        spectrum[which, 1] = -(both[:extent, extent:] + both[extent:, :extent])

    @pl.loop(0, own)
    def _(which):
        @pl.loop(1, spread)
        def _(step):
            to, source = peer(step)
            phase_copy(which, step, to, source).wait_recv()

        cosine, sine = cos_sin(phase[which])
        scale = 1.0 / float(extent * extent)
        real, imag = spectrum[which, 0] * scale, spectrum[which, 1] * scale
        moved = jnp.concatenate([real * cosine - imag * sine, real * sine + imag * cosine], axis=1)
        both = apply_left(table[...], moved)
        back = jnp.concatenate(
            [both[:extent, :extent] - both[extent:, extent:], both[:extent, extent:] + both[extent:, :extent]], axis=0
        )
        both = apply_left_transposed(table[...], back)
        field_real = both[:extent, :extent] - both[extent:, extent:]
        field_imag = both[:extent, extent:] + both[extent:, :extent]
        intensity[which] = field_real * field_real + field_imag * field_imag

        @pl.when(which < own - 1)
        def _():
            @pl.loop(1, spread)
            def _(turn):
                step = spread - turn
                out_copy(which, step, peer(step)[0], me_d).start()

        @pl.when(which == own - 1)
        def _():
            for low, high in zip(EDGES, EDGES[1:]):

                @pl.loop(1, spread)
                def _(turn):
                    step = spread - turn
                    to = peer(step)[0]

                    @pl.when((to * 8 >= low * spread) & (to * 8 < high * spread))
                    def _():
                        out_copy(which, step, to, me_d).start()

        pltpu.make_async_copy(
            intensity.at[which, pl.ds(me_d * rows, rows), :], out.at[me_d * own + which], local_sem.at[4 + which]
        ).start()

    @pl.loop(1, side)
    def _(shift):
        row_copy(shift, me_t).wait_send()
        want_copy(shift, me_y).wait_send()

    @pl.loop(1, tiles)
    def _(step):
        to, source = shifted(step // side, step % side)
        pack_copy(step, to, source).wait_send()

    @pl.loop(1, spread)
    def _(step):
        to, source = peer(step)
        pixel_copy(step, to, source).wait_send()

    @pl.loop(0, own)
    def _(which):
        @pl.loop(1, spread)
        def _(step):
            to, source = peer(step)
            phase_copy(which, step, to, source).wait_send()
            out_copy(which, step, to, source).wait()

        pltpu.make_async_copy(
            intensity.at[which, pl.ds(me_d * rows, rows), :], out.at[me_d * own + which], local_sem.at[4 + which]
        ).wait()


def solution(mesh):
    tiles, spread = mesh.shape["tile"], mesh.shape["depth"]

    def on_device(patches, patch_owner, patch_level, phases):
        count, rows, extent = patches.shape
        own = count // spread
        depth_count = phases.shape[0]
        ring_rounds, side = reaches(spread)[1], math.isqrt(tiles)
        tables = jnp.asarray(dft_tables(extent))
        any_space = pl.BlockSpec(memory_space=pl.ANY)
        scalars = pl.BlockSpec(memory_space=pltpu.SMEM)
        f32, dma = jnp.float32, pltpu.SemaphoreType.DMA
        return pl.pallas_call(
            functools.partial(kernel, tiles),
            out_shape=pltpu.VMEM(patches.shape, patches.dtype),
            in_specs=[any_space, scalars, scalars, any_space, any_space],
            out_specs=pl.BlockSpec(memory_space=pltpu.VMEM),
            scratch_shapes=[
                pltpu.VMEM(tables.shape, tables.dtype),
                pltpu.VMEM((depth_count, rows, extent), f32),
                pltpu.VMEM((1, LANES), jnp.int32),
                pltpu.SMEM((1, LANES), jnp.int32),
                pltpu.VMEM((1, LANES), jnp.int32),
                pltpu.VMEM((tiles, 1, LANES), jnp.int32),
                pltpu.SMEM((tiles, 1, LANES), jnp.int32),
                pltpu.VMEM((tiles, CAP, rows, extent), f32),
                pltpu.VMEM((tiles * CAP, rows, extent), f32),
                pltpu.VMEM((own, spread, rows, extent), f32),
                pltpu.VMEM((own, extent, extent), f32),
                pltpu.VMEM((own, extent, extent), f32),
                pltpu.VMEM((own, 2, extent, extent), f32),
                pltpu.VMEM((own, extent, extent), f32),
                pltpu.SemaphoreType.REGULAR((ring_rounds, 2)),
                dma((4 + own,)),
                dma((side,)),
                dma((side,)),
                dma((side,)),
                dma((side,)),
                dma((tiles,)),
                dma((tiles,)),
                dma((spread,)),
                dma((spread,)),
                dma((own, spread)),
                dma((own, spread)),
                dma((own, spread)),
                dma((own, spread)),
            ],
            compiler_params=pltpu.CompilerParams(
                collective_id=0, has_side_effects=True, vmem_limit_bytes=60 * 1024 * 1024
            ),
        )(
            patches,
            patch_owner.reshape(1, count),
            patch_level.reshape(1, count),
            jnp.transpose(phases, (0, 2, 1)),
            tables,
        )

    return jax.shard_map(
        on_device,
        mesh=mesh,
        in_specs=(P("tile", "depth", None), P("tile", None), P("tile"), P("tile", None, "depth")),
        out_specs=P("tile", "depth", None),
        check_vma=False,
    )
```

```python
import functools
import math

import jax
import jax.numpy as jnp
import numpy as np
from jax import lax
from jax.experimental import pallas as pl
from jax.experimental.pallas import tpu as pltpu
from jax.sharding import PartitionSpec as P

CAP = 8
LANES = 128
EDGES = (0, 1, 2, 3, 4, 5, 6, 7, 8)


def dft_tables(extent):
    indices = np.arange(extent)
    angles = (indices[:, None] * indices[None, :] % extent) * (2.0 * math.pi / extent)
    exact = np.concatenate([np.cos(angles), np.sin(angles)], axis=0)
    high = exact.astype(np.float32).astype(jnp.bfloat16)
    low = (exact - high.astype(np.float64)).astype(np.float32).astype(jnp.bfloat16)
    return np.concatenate([high, low, high], axis=1)


def split(values):
    high = values.astype(jnp.bfloat16)
    low = (values - high.astype(jnp.float32)).astype(jnp.bfloat16)
    return high, low


def apply_left(table, values):
    high, low = split(values)
    stacked = jnp.concatenate([high, high, low], axis=0)
    return jnp.dot(table, stacked, preferred_element_type=jnp.float32)


def apply_left_transposed(table, values):
    high, low = split(values)
    stacked = jnp.concatenate([high, high, low], axis=1)
    return lax.dot_general(table, stacked, (((1,), (1,)), ((), ())), preferred_element_type=jnp.float32)


def polynomial(square, terms):
    total = jnp.full_like(square, terms[-1])
    for term in terms[-2::-1]:
        total = total * square + term
    return total


SIN_TERMS = [(-1.0) ** n / math.factorial(2 * n + 1) for n in range(7)]
COS_TERMS = [(-1.0) ** n / math.factorial(2 * n) for n in range(8)]


def cos_sin(phase):
    half = phase * 0.5
    square = half * half
    sine = half * polynomial(square, SIN_TERMS)
    cosine = polynomial(square, COS_TERMS)
    return 1.0 - 2.0 * sine * sine, 2.0 * sine * cosine


def near_first(step):
    return ((step + 1) // 2) * (2 * (step % 2) - 1)


def reaches(spread):
    half = spread // 4
    reach = max(1, half // 4)
    return reach, -(-(half - reach) // reach)


def kernel(
    tiles,
    patches,
    owner,
    level,
    phases,
    tables,
    out,
    table,
    depths,
    slot_row,
    slot_at,
    want_row,
    wants,
    wants_at,
    packed,
    got,
    chosen,
    pixels,
    phase,
    spectrum,
    intensity,
    ring_sem,
    local_sem,
    row_send,
    row_recv,
    want_send,
    want_recv,
    pack_send,
    pack_recv,
    pixel_send,
    pixel_recv,
    phase_send,
    phase_recv,
    out_send,
    out_recv,
):
    count, rows, extent = patches.shape
    spread = extent // rows
    ring = spread // 2
    own = count // spread
    side = math.isqrt(tiles)
    me_t, me_d = lax.axis_index("tile"), lax.axis_index("depth")
    me_y, me_x, me_z, me_c = me_t // side, me_t % side, me_d // 2, me_d % 2

    def peer(step):
        hop, swap = near_first(step // 2), step % 2
        to = ((me_z + ring + hop) % ring) * 2 + (me_c + swap) % 2
        source = ((me_z + ring - hop) % ring) * 2 + (me_c + swap) % 2
        return to, source

    def shifted(down, over):
        to = ((me_y + down) % side) * side + (me_x + over) % side
        source = ((me_y + side - down) % side) * side + (me_x + side - over) % side
        return to, source

    reach, ring_rounds = reaches(spread)

    def within(distance):
        return min(2 * (2 * distance + 1), spread)

    barrier = pltpu.get_barrier_semaphore()

    @pl.loop(1, within(reach))
    def _(step):
        pl.semaphore_signal(barrier, inc=1, device_id={"depth": peer(step)[0]})

    @pl.loop(1, side)
    def _(shift):
        pl.semaphore_signal(barrier, inc=1, device_id={"tile": shifted(0, shift)[0]})
        pl.semaphore_signal(barrier, inc=1, device_id={"tile": shifted(shift, 0)[0]})

    def tell_ring(turn):
        for way, hop in enumerate((reach, ring - reach)):
            to = ((me_z + hop) % ring) * 2 + me_c
            pl.semaphore_signal(ring_sem.at[turn, way], inc=1, device_id={"depth": to})

    def learn_ring(turn):
        for way in range(2):
            pl.semaphore_wait(ring_sem.at[turn, way], 1)
        if turn + 1 < ring_rounds:
            tell_ring(turn + 1)
        send_pixels(turn + 1)

    load_depths = pltpu.make_async_copy(phases, depths, local_sem.at[0])
    load_depths.start()
    load_table = pltpu.make_async_copy(tables, table, local_sem.at[1])
    load_table.start()
    load_pixels = pltpu.make_async_copy(
        patches.at[pl.ds(me_d * own, own)], pixels.at[:, pl.ds(me_d * rows, rows), :], local_sem.at[2]
    )
    load_pixels.start()

    lane = lax.broadcasted_iota(jnp.int32, (1, LANES), 1)
    owners = lax.fori_loop(
        0, count, lambda p, row: jnp.where(lane == p, owner[0, p], row), jnp.full((1, LANES), -1, jnp.int32)
    )
    ranks = lax.fori_loop(
        0,
        count,
        lambda p, row: row + jnp.where((owners == owner[0, p]) & (lane > p), 1, 0),
        jnp.zeros((1, LANES), jnp.int32),
    )
    slot_row[...] = owners * CAP + ranks
    load_slots = pltpu.make_async_copy(slot_row, slot_at, local_sem.at[3])
    load_slots.start()
    load_slots.wait()
    wanted = lax.fori_loop(
        0,
        count,
        lambda p, row: jnp.where(lane == slot_at[0, p], level[0, p], row),
        jnp.zeros((1, LANES), jnp.int32),
    )
    want_row[...] = wanted
    wants[me_t] = wanted

    pl.semaphore_wait(barrier, within(reach) - 1 + 2 * (side - 1))
    tell_ring(0)

    def row_copy(shift, source):
        return pltpu.make_async_remote_copy(
            src_ref=want_row,
            dst_ref=wants.at[source],
            send_sem=row_send.at[shift],
            recv_sem=row_recv.at[shift],
            device_id={"tile": shifted(0, shift)[0]},
        )

    def want_copy(shift, source_row):
        return pltpu.make_async_remote_copy(
            src_ref=wants.at[pl.ds(me_y * side, side)],
            dst_ref=wants.at[pl.ds(source_row * side, side)],
            send_sem=want_send.at[shift],
            recv_sem=want_recv.at[shift],
            device_id={"tile": shifted(shift, 0)[0]},
        )

    def pixel_copy(step, to, source):
        return pltpu.make_async_remote_copy(
            src_ref=patches.at[pl.ds(to * own, own)],
            dst_ref=pixels.at[:, pl.ds(source * rows, rows), :],
            send_sem=pixel_send.at[step],
            recv_sem=pixel_recv.at[step],
            device_id={"depth": to},
        )

    def pack_copy(step, to, source):
        return pltpu.make_async_remote_copy(
            src_ref=packed.at[to],
            dst_ref=got.at[pl.ds(source * CAP, CAP)],
            send_sem=pack_send.at[step],
            recv_sem=pack_recv.at[step],
            device_id={"tile": to},
        )

    def phase_copy(which, step, to, source):
        return pltpu.make_async_remote_copy(
            src_ref=chosen.at[which, to],
            dst_ref=phase.at[which, pl.ds(source * rows, rows), :],
            send_sem=phase_send.at[which, step],
            recv_sem=phase_recv.at[which, step],
            device_id={"depth": to},
        )

    def out_copy(which, step, to, source):
        return pltpu.make_async_remote_copy(
            src_ref=intensity.at[which, pl.ds(to * rows, rows), :],
            dst_ref=out.at[source * own + which],
            send_sem=out_send.at[which, step],
            recv_sem=out_recv.at[which, step],
            device_id={"depth": to},
        )

    def send_pixels(turn):
        first = 1 if turn == 0 else within(turn * reach)

        @pl.loop(first, within((turn + 1) * reach))
        def _(step):
            pixel_copy(step, peer(step)[0], me_d).start()

    def send_packed(down, over):
        to = shifted(down, over)[0]
        for slot in range(CAP):
            packed[to, slot] = depths[wants_at[to, 0, me_t * CAP + slot]]
        pack_copy(down * side + over, to, me_t).start()

    def read_wants(row):
        load = pltpu.make_async_copy(
            wants.at[pl.ds(row * side, side)], wants_at.at[pl.ds(row * side, side)], local_sem.at[3]
        )
        load.start()
        load.wait()

    @pl.loop(1, side)
    def _(shift):
        row_copy(shift, me_t).start()

    send_pixels(0)
    learn_ring(0)

    @pl.loop(1, side)
    def _(shift):
        row_copy(shift, shifted(0, shift)[1]).wait_recv()

    @pl.loop(1, side)
    def _(shift):
        want_copy(shift, me_y).start()

    for turn in range(1, ring_rounds):
        learn_ring(turn)
    load_depths.wait()
    read_wants(me_y)

    @pl.loop(1, side)
    def _(over):
        send_packed(0, over)

    @pl.loop(1, side)
    def _(turn):
        down = (side + near_first(turn)) % side
        want_copy(side - down, (me_y + down) % side).wait_recv()
        read_wants((me_y + down) % side)

        @pl.loop(0, side)
        def _(over):
            send_packed(down, over)

    for slot in range(CAP):
        got[me_t * CAP + slot] = depths[wants_at[me_t, 0, me_t * CAP + slot]]

    @pl.loop(1, tiles)
    def _(step):
        to, source = shifted(step // side, step % side)
        pack_copy(step, to, source).wait_recv()

    @pl.loop(0, own)
    def _(which):
        @pl.loop(1, spread)
        def _(turn):
            step = spread - turn
            to = peer(step)[0]
            chosen[which, to] = got[slot_at[0, to * own + which]]
            phase_copy(which, step, to, me_d).start()

        phase[which, pl.ds(me_d * rows, rows), :] = got[slot_at[0, me_d * own + which]]

    load_table.wait()
    load_pixels.wait()

    @pl.loop(1, spread)
    def _(step):
        to, source = peer(step)
        pixel_copy(step, to, source).wait_recv()

    @pl.loop(0, own)
    def _(which):
        columns = apply_left(table[...], pixels[which])
        both = apply_left_transposed(table[...], columns)
        spectrum[which, 0] = both[:extent, :extent] - both[extent:, extent:]
        spectrum[which, 1] = -(both[:extent, extent:] + both[extent:, :extent])

    @pl.loop(0, own)
    def _(which):
        @pl.loop(1, spread)
        def _(step):
            to, source = peer(step)
            phase_copy(which, step, to, source).wait_recv()

        cosine, sine = cos_sin(phase[which])
        scale = 1.0 / float(extent * extent)
        real, imag = spectrum[which, 0] * scale, spectrum[which, 1] * scale
        moved = jnp.concatenate([real * cosine - imag * sine, real * sine + imag * cosine], axis=1)
        both = apply_left(table[...], moved)
        back = jnp.concatenate(
            [both[:extent, :extent] - both[extent:, extent:], both[:extent, extent:] + both[extent:, :extent]], axis=0
        )
        both = apply_left_transposed(table[...], back)
        field_real = both[:extent, :extent] - both[extent:, extent:]
        field_imag = both[:extent, extent:] + both[extent:, :extent]
        intensity[which] = field_real * field_real + field_imag * field_imag

        @pl.when(which < own - 1)
        def _():
            @pl.loop(1, spread)
            def _(turn):
                step = spread - turn
                out_copy(which, step, peer(step)[0], me_d).start()

        @pl.when(which == own - 1)
        def _():
            for low, high in zip(EDGES, EDGES[1:]):

                @pl.loop(1, spread)
                def _(turn):
                    step = spread - turn
                    to = peer(step)[0]

                    @pl.when((to * 8 >= low * spread) & (to * 8 < high * spread))
                    def _():
                        out_copy(which, step, to, me_d).start()

        pltpu.make_async_copy(
            intensity.at[which, pl.ds(me_d * rows, rows), :], out.at[me_d * own + which], local_sem.at[4 + which]
        ).start()

    @pl.loop(1, side)
    def _(shift):
        row_copy(shift, me_t).wait_send()
        want_copy(shift, me_y).wait_send()

    @pl.loop(1, tiles)
    def _(step):
        to, source = shifted(step // side, step % side)
        pack_copy(step, to, source).wait_send()

    @pl.loop(1, spread)
    def _(step):
        to, source = peer(step)
        pixel_copy(step, to, source).wait_send()

    @pl.loop(0, own)
    def _(which):
        @pl.loop(1, spread)
        def _(step):
            to, source = peer(step)
            phase_copy(which, step, to, source).wait_send()
            out_copy(which, step, to, source).wait()

        pltpu.make_async_copy(
            intensity.at[which, pl.ds(me_d * rows, rows), :], out.at[me_d * own + which], local_sem.at[4 + which]
        ).wait()


def solution(mesh):
    tiles, spread = mesh.shape["tile"], mesh.shape["depth"]

    def on_device(patches, patch_owner, patch_level, phases):
        count, rows, extent = patches.shape
        own = count // spread
        depth_count = phases.shape[0]
        ring_rounds, side = reaches(spread)[1], math.isqrt(tiles)
        tables = jnp.asarray(dft_tables(extent))
        any_space = pl.BlockSpec(memory_space=pl.ANY)
        scalars = pl.BlockSpec(memory_space=pltpu.SMEM)
        f32, dma = jnp.float32, pltpu.SemaphoreType.DMA
        return pl.pallas_call(
            functools.partial(kernel, tiles),
            out_shape=pltpu.VMEM(patches.shape, patches.dtype),
            in_specs=[any_space, scalars, scalars, any_space, any_space],
            out_specs=pl.BlockSpec(memory_space=pltpu.VMEM),
            scratch_shapes=[
                pltpu.VMEM(tables.shape, tables.dtype),
                pltpu.VMEM((depth_count, rows, extent), f32),
                pltpu.VMEM((1, LANES), jnp.int32),
                pltpu.SMEM((1, LANES), jnp.int32),
                pltpu.VMEM((1, LANES), jnp.int32),
                pltpu.VMEM((tiles, 1, LANES), jnp.int32),
                pltpu.SMEM((tiles, 1, LANES), jnp.int32),
                pltpu.VMEM((tiles, CAP, rows, extent), f32),
                pltpu.VMEM((tiles * CAP, rows, extent), f32),
                pltpu.VMEM((own, spread, rows, extent), f32),
                pltpu.VMEM((own, extent, extent), f32),
                pltpu.VMEM((own, extent, extent), f32),
                pltpu.VMEM((own, 2, extent, extent), f32),
                pltpu.VMEM((own, extent, extent), f32),
                pltpu.SemaphoreType.REGULAR((ring_rounds, 2)),
                dma((4 + own,)),
                dma((side,)),
                dma((side,)),
                dma((side,)),
                dma((side,)),
                dma((tiles,)),
                dma((tiles,)),
                dma((spread,)),
                dma((spread,)),
                dma((own, spread)),
                dma((own, spread)),
                dma((own, spread)),
                dma((own, spread)),
            ],
            compiler_params=pltpu.CompilerParams(
                collective_id=0, has_side_effects=True, vmem_limit_bytes=60 * 1024 * 1024
            ),
        )(
            patches,
            patch_owner.reshape(1, count),
            patch_level.reshape(1, count),
            jnp.transpose(phases, (0, 2, 1)),
            tables,
        )

    return jax.shard_map(
        on_device,
        mesh=mesh,
        in_specs=(P("tile", "depth", None), P("tile", None), P("tile"), P("tile", None, "depth")),
        out_specs=P("tile", "depth", None),
        check_vma=False,
    )
```

```python
import functools
import math

import jax
import jax.numpy as jnp
import numpy as np
from jax import lax
from jax.experimental import pallas as pl
from jax.experimental.pallas import tpu as pltpu
from jax.sharding import PartitionSpec as P

CAP = 8
LANES = 128
EDGES = (0, 1, 2, 3, 4, 5, 6, 7, 8)


def dft_tables(extent):
    indices = np.arange(extent)
    angles = (indices[:, None] * indices[None, :] % extent) * (2.0 * math.pi / extent)
    exact = np.concatenate([np.cos(angles), np.sin(angles)], axis=0)
    high = exact.astype(np.float32).astype(jnp.bfloat16)
    low = (exact - high.astype(np.float64)).astype(np.float32).astype(jnp.bfloat16)
    return np.concatenate([high, low, high], axis=1)


def split(values):
    high = values.astype(jnp.bfloat16)
    low = (values - high.astype(jnp.float32)).astype(jnp.bfloat16)
    return high, low


def apply_left(table, values):
    high, low = split(values)
    stacked = jnp.concatenate([high, high, low], axis=0)
    return jnp.dot(table, stacked, preferred_element_type=jnp.float32)


def apply_left_transposed(table, values):
    high, low = split(values)
    stacked = jnp.concatenate([high, high, low], axis=1)
    return lax.dot_general(table, stacked, (((1,), (1,)), ((), ())), preferred_element_type=jnp.float32)


def polynomial(square, terms):
    total = jnp.full_like(square, terms[-1])
    for term in terms[-2::-1]:
        total = total * square + term
    return total


SIN_TERMS = [(-1.0) ** n / math.factorial(2 * n + 1) for n in range(7)]
COS_TERMS = [(-1.0) ** n / math.factorial(2 * n) for n in range(8)]


def cos_sin(phase):
    half = phase * 0.5
    square = half * half
    sine = half * polynomial(square, SIN_TERMS)
    cosine = polynomial(square, COS_TERMS)
    return 1.0 - 2.0 * sine * sine, 2.0 * sine * cosine


def near_first(step):
    return ((step + 1) // 2) * (2 * (step % 2) - 1)


def reaches(spread):
    half = spread // 4
    reach = max(1, half // 4)
    return reach, -(-(half - reach) // reach)


def kernel(
    tiles,
    patches,
    owners_in,
    levels_in,
    phases,
    tables,
    out,
    table,
    held,
    depths,
    owner,
    level,
    slot_row,
    slot_at,
    want_row,
    wants,
    wants_at,
    packed,
    got,
    chosen,
    pixels,
    phase,
    spectrum,
    intensity,
    ring_sem,
    local_sem,
    row_send,
    row_recv,
    want_send,
    want_recv,
    pack_send,
    pack_recv,
    pixel_send,
    pixel_recv,
    phase_send,
    phase_recv,
    out_send,
    out_recv,
):
    count, rows, extent = patches.shape
    spread = extent // rows
    ring = spread // 2
    own = count // spread
    side = math.isqrt(tiles)
    me_t, me_d = lax.axis_index("tile"), lax.axis_index("depth")
    me_y, me_x, me_z, me_c = me_t // side, me_t % side, me_d // 2, me_d % 2

    def peer(step):
        hop, swap = near_first(step // 2), step % 2
        to = ((me_z + ring + hop) % ring) * 2 + (me_c + swap) % 2
        source = ((me_z + ring - hop) % ring) * 2 + (me_c + swap) % 2
        return to, source

    def shifted(down, over):
        to = ((me_y + down) % side) * side + (me_x + over) % side
        source = ((me_y + side - down) % side) * side + (me_x + side - over) % side
        return to, source

    reach, ring_rounds = reaches(spread)

    def within(distance):
        return min(2 * (2 * distance + 1), spread)

    barrier = pltpu.get_barrier_semaphore()

    @pl.loop(1, within(reach))
    def _(step):
        pl.semaphore_signal(barrier, inc=1, device_id={"depth": peer(step)[0]})

    @pl.loop(1, side)
    def _(shift):
        pl.semaphore_signal(barrier, inc=1, device_id={"tile": shifted(0, shift)[0]})
        pl.semaphore_signal(barrier, inc=1, device_id={"tile": shifted(shift, 0)[0]})

    def tell_ring(turn):
        for way, hop in enumerate((reach, ring - reach)):
            to = ((me_z + hop) % ring) * 2 + me_c
            pl.semaphore_signal(ring_sem.at[turn, way], inc=1, device_id={"depth": to})

    def learn_ring(turn):
        for way in range(2):
            pl.semaphore_wait(ring_sem.at[turn, way], 1)
        if turn + 1 < ring_rounds:
            tell_ring(turn + 1)
        send_pixels(turn + 1)

    load_owner = pltpu.make_async_copy(owners_in, owner, local_sem.at[3])
    load_owner.start()
    load_level = pltpu.make_async_copy(levels_in, level, local_sem.at[4 + own])
    load_level.start()
    load_held = pltpu.make_async_copy(patches, held, local_sem.at[5 + own])
    load_held.start()
    load_depths = pltpu.make_async_copy(phases, depths, local_sem.at[0])
    load_depths.start()
    load_table = pltpu.make_async_copy(tables, table, local_sem.at[1])
    load_table.start()
    load_pixels = pltpu.make_async_copy(
        patches.at[pl.ds(me_d * own, own)], pixels.at[:, pl.ds(me_d * rows, rows), :], local_sem.at[2]
    )
    load_pixels.start()

    load_owner.wait()
    load_level.wait()

    lane = lax.broadcasted_iota(jnp.int32, (1, LANES), 1)
    owners = lax.fori_loop(
        0, count, lambda p, row: jnp.where(lane == p, owner[0, p], row), jnp.full((1, LANES), -1, jnp.int32)
    )
    ranks = lax.fori_loop(
        0,
        count,
        lambda p, row: row + jnp.where((owners == owner[0, p]) & (lane > p), 1, 0),
        jnp.zeros((1, LANES), jnp.int32),
    )
    slot_row[...] = owners * CAP + ranks
    load_slots = pltpu.make_async_copy(slot_row, slot_at, local_sem.at[3])
    load_slots.start()
    load_slots.wait()
    wanted = lax.fori_loop(
        0,
        count,
        lambda p, row: jnp.where(lane == slot_at[0, p], level[0, p], row),
        jnp.zeros((1, LANES), jnp.int32),
    )
    want_row[...] = wanted
    wants[me_t] = wanted

    pl.semaphore_wait(barrier, within(reach) - 1 + 2 * (side - 1))
    tell_ring(0)

    def row_copy(shift, source):
        return pltpu.make_async_remote_copy(
            src_ref=want_row,
            dst_ref=wants.at[source],
            send_sem=row_send.at[shift],
            recv_sem=row_recv.at[shift],
            device_id={"tile": shifted(0, shift)[0]},
        )

    def want_copy(shift, source_row):
        return pltpu.make_async_remote_copy(
            src_ref=wants.at[pl.ds(me_y * side, side)],
            dst_ref=wants.at[pl.ds(source_row * side, side)],
            send_sem=want_send.at[shift],
            recv_sem=want_recv.at[shift],
            device_id={"tile": shifted(shift, 0)[0]},
        )

    def pixel_copy(step, to, source):
        return pltpu.make_async_remote_copy(
            src_ref=held.at[pl.ds(to * own, own)],
            dst_ref=pixels.at[:, pl.ds(source * rows, rows), :],
            send_sem=pixel_send.at[step],
            recv_sem=pixel_recv.at[step],
            device_id={"depth": to},
        )

    def pack_copy(step, to, source):
        return pltpu.make_async_remote_copy(
            src_ref=packed.at[to],
            dst_ref=got.at[pl.ds(source * CAP, CAP)],
            send_sem=pack_send.at[step],
            recv_sem=pack_recv.at[step],
            device_id={"tile": to},
        )

    def phase_copy(which, step, to, source):
        return pltpu.make_async_remote_copy(
            src_ref=chosen.at[which, to],
            dst_ref=phase.at[which, pl.ds(source * rows, rows), :],
            send_sem=phase_send.at[which, step],
            recv_sem=phase_recv.at[which, step],
            device_id={"depth": to},
        )

    def out_copy(which, step, to, source):
        return pltpu.make_async_remote_copy(
            src_ref=intensity.at[which, pl.ds(to * rows, rows), :],
            dst_ref=out.at[source * own + which],
            send_sem=out_send.at[which, step],
            recv_sem=out_recv.at[which, step],
            device_id={"depth": to},
        )

    def send_pixels(turn):
        first = 1 if turn == 0 else within(turn * reach)

        @pl.loop(first, within((turn + 1) * reach))
        def _(step):
            pixel_copy(step, peer(step)[0], me_d).start()

    def send_packed(down, over):
        to = shifted(down, over)[0]
        for slot in range(CAP):
            packed[to, slot] = depths[wants_at[to, 0, me_t * CAP + slot]]
        pack_copy(down * side + over, to, me_t).start()

    def read_wants(row):
        load = pltpu.make_async_copy(
            wants.at[pl.ds(row * side, side)], wants_at.at[pl.ds(row * side, side)], local_sem.at[3]
        )
        load.start()
        load.wait()

    @pl.loop(1, side)
    def _(shift):
        row_copy(shift, me_t).start()

    load_held.wait()
    send_pixels(0)
    learn_ring(0)

    @pl.loop(1, side)
    def _(shift):
        row_copy(shift, shifted(0, shift)[1]).wait_recv()

    @pl.loop(1, side)
    def _(shift):
        want_copy(shift, me_y).start()

    for turn in range(1, ring_rounds):
        learn_ring(turn)
    load_depths.wait()
    read_wants(me_y)

    @pl.loop(1, side)
    def _(over):
        send_packed(0, over)

    @pl.loop(1, side)
    def _(turn):
        down = (side + near_first(turn)) % side
        want_copy(side - down, (me_y + down) % side).wait_recv()
        read_wants((me_y + down) % side)

        @pl.loop(0, side)
        def _(over):
            send_packed(down, over)

    for slot in range(CAP):
        got[me_t * CAP + slot] = depths[wants_at[me_t, 0, me_t * CAP + slot]]

    @pl.loop(1, tiles)
    def _(step):
        to, source = shifted(step // side, step % side)
        pack_copy(step, to, source).wait_recv()

    @pl.loop(0, own)
    def _(which):
        @pl.loop(1, spread)
        def _(turn):
            step = spread - turn
            to = peer(step)[0]
            chosen[which, to] = got[slot_at[0, to * own + which]]
            phase_copy(which, step, to, me_d).start()

        phase[which, pl.ds(me_d * rows, rows), :] = got[slot_at[0, me_d * own + which]]

    load_table.wait()
    load_pixels.wait()

    @pl.loop(1, spread)
    def _(step):
        to, source = peer(step)
        pixel_copy(step, to, source).wait_recv()

    @pl.loop(0, own)
    def _(which):
        columns = apply_left(table[...], pixels[which])
        both = apply_left_transposed(table[...], columns)
        spectrum[which, 0] = both[:extent, :extent] - both[extent:, extent:]
        spectrum[which, 1] = -(both[:extent, extent:] + both[extent:, :extent])

    @pl.loop(0, own)
    def _(which):
        @pl.loop(1, spread)
        def _(step):
            to, source = peer(step)
            phase_copy(which, step, to, source).wait_recv()

        cosine, sine = cos_sin(phase[which])
        scale = 1.0 / float(extent * extent)
        real, imag = spectrum[which, 0] * scale, spectrum[which, 1] * scale
        moved = jnp.concatenate([real * cosine - imag * sine, real * sine + imag * cosine], axis=1)
        both = apply_left(table[...], moved)
        back = jnp.concatenate(
            [both[:extent, :extent] - both[extent:, extent:], both[:extent, extent:] + both[extent:, :extent]], axis=0
        )
        both = apply_left_transposed(table[...], back)
        field_real = both[:extent, :extent] - both[extent:, extent:]
        field_imag = both[:extent, extent:] + both[extent:, :extent]
        intensity[which] = field_real * field_real + field_imag * field_imag

        @pl.when(which < own - 1)
        def _():
            @pl.loop(1, spread)
            def _(turn):
                step = spread - turn
                out_copy(which, step, peer(step)[0], me_d).start()

        @pl.when(which == own - 1)
        def _():
            for low, high in zip(EDGES, EDGES[1:]):

                @pl.loop(1, spread)
                def _(turn):
                    step = spread - turn
                    to = peer(step)[0]

                    @pl.when((to * 8 >= low * spread) & (to * 8 < high * spread))
                    def _():
                        out_copy(which, step, to, me_d).start()

        pltpu.make_async_copy(
            intensity.at[which, pl.ds(me_d * rows, rows), :], out.at[me_d * own + which], local_sem.at[4 + which]
        ).start()

    @pl.loop(1, side)
    def _(shift):
        row_copy(shift, me_t).wait_send()
        want_copy(shift, me_y).wait_send()

    @pl.loop(1, tiles)
    def _(step):
        to, source = shifted(step // side, step % side)
        pack_copy(step, to, source).wait_send()

    @pl.loop(1, spread)
    def _(step):
        to, source = peer(step)
        pixel_copy(step, to, source).wait_send()

    @pl.loop(0, own)
    def _(which):
        @pl.loop(1, spread)
        def _(step):
            to, source = peer(step)
            phase_copy(which, step, to, source).wait_send()
            out_copy(which, step, to, source).wait()

        pltpu.make_async_copy(
            intensity.at[which, pl.ds(me_d * rows, rows), :], out.at[me_d * own + which], local_sem.at[4 + which]
        ).wait()


def solution(mesh):
    tiles, spread = mesh.shape["tile"], mesh.shape["depth"]

    def on_device(patches, patch_owner, patch_level, phases):
        count, rows, extent = patches.shape
        own = count // spread
        depth_count = phases.shape[0]
        ring_rounds, side = reaches(spread)[1], math.isqrt(tiles)
        tables = jnp.asarray(dft_tables(extent))
        any_space = pl.BlockSpec(memory_space=pl.ANY)
        f32, dma = jnp.float32, pltpu.SemaphoreType.DMA
        return pl.pallas_call(
            functools.partial(kernel, tiles),
            out_shape=pltpu.VMEM(patches.shape, patches.dtype),
            in_specs=[any_space] * 5,
            out_specs=pl.BlockSpec(memory_space=pltpu.VMEM),
            scratch_shapes=[
                pltpu.VMEM(tables.shape, tables.dtype),
                pltpu.VMEM(patches.shape, f32),
                pltpu.VMEM((depth_count, rows, extent), f32),
                pltpu.SMEM((1, count), jnp.int32),
                pltpu.SMEM((1, count), jnp.int32),
                pltpu.VMEM((1, LANES), jnp.int32),
                pltpu.SMEM((1, LANES), jnp.int32),
                pltpu.VMEM((1, LANES), jnp.int32),
                pltpu.VMEM((tiles, 1, LANES), jnp.int32),
                pltpu.SMEM((tiles, 1, LANES), jnp.int32),
                pltpu.VMEM((tiles, CAP, rows, extent), f32),
                pltpu.VMEM((tiles * CAP, rows, extent), f32),
                pltpu.VMEM((own, spread, rows, extent), f32),
                pltpu.VMEM((own, extent, extent), f32),
                pltpu.VMEM((own, extent, extent), f32),
                pltpu.VMEM((own, 2, extent, extent), f32),
                pltpu.VMEM((own, extent, extent), f32),
                pltpu.SemaphoreType.REGULAR((ring_rounds, 2)),
                dma((6 + own,)),
                dma((side,)),
                dma((side,)),
                dma((side,)),
                dma((side,)),
                dma((tiles,)),
                dma((tiles,)),
                dma((spread,)),
                dma((spread,)),
                dma((own, spread)),
                dma((own, spread)),
                dma((own, spread)),
                dma((own, spread)),
            ],
            compiler_params=pltpu.CompilerParams(
                collective_id=0, has_side_effects=True, vmem_limit_bytes=60 * 1024 * 1024
            ),
        )(
            patches,
            patch_owner.reshape(1, count),
            patch_level.reshape(1, count),
            jnp.transpose(phases, (0, 2, 1)),
            tables,
        )

    return jax.shard_map(
        on_device,
        mesh=mesh,
        in_specs=(P("tile", "depth", None), P("tile", None), P("tile"), P("tile", None, "depth")),
        out_specs=P("tile", "depth", None),
        check_vma=False,
    )
```

```python
import functools
import math

import jax
import jax.numpy as jnp
import numpy as np
from jax import lax
from jax.experimental import pallas as pl
from jax.experimental.pallas import tpu as pltpu
from jax.sharding import PartitionSpec as P

CAP = 8
LANES = 128
EDGES = (0, 1, 2, 3, 4, 5, 6, 7, 8)


def dft_tables(extent):
    indices = np.arange(extent)
    angles = (indices[:, None] * indices[None, :] % extent) * (2.0 * math.pi / extent)
    exact = np.concatenate([np.cos(angles), np.sin(angles)], axis=0)
    high = exact.astype(np.float32).astype(jnp.bfloat16)
    low = (exact - high.astype(np.float64)).astype(np.float32).astype(jnp.bfloat16)
    return np.concatenate([high, low, high], axis=1)


def split(values):
    high = values.astype(jnp.bfloat16)
    low = (values - high.astype(jnp.float32)).astype(jnp.bfloat16)
    return high, low


def apply_left(table, values):
    high, low = split(values)
    stacked = jnp.concatenate([high, high, low], axis=0)
    return jnp.dot(table, stacked, preferred_element_type=jnp.float32)


def apply_left_transposed(table, values):
    high, low = split(values)
    stacked = jnp.concatenate([high, high, low], axis=1)
    return lax.dot_general(table, stacked, (((1,), (1,)), ((), ())), preferred_element_type=jnp.float32)


def polynomial(square, terms):
    total = jnp.full_like(square, terms[-1])
    for term in terms[-2::-1]:
        total = total * square + term
    return total


SIN_TERMS = [(-1.0) ** n / math.factorial(2 * n + 1) for n in range(7)]
COS_TERMS = [(-1.0) ** n / math.factorial(2 * n) for n in range(8)]


def cos_sin(phase):
    half = phase * 0.5
    square = half * half
    sine = half * polynomial(square, SIN_TERMS)
    cosine = polynomial(square, COS_TERMS)
    return 1.0 - 2.0 * sine * sine, 2.0 * sine * cosine


def near_first(step):
    return ((step + 1) // 2) * (2 * (step % 2) - 1)


def reaches(spread):
    half = spread // 4
    reach = max(1, half // 4)
    return reach, -(-(half - reach) // reach)


def kernel(
    tiles,
    patches,
    owners_in,
    levels_in,
    phases,
    tables,
    out,
    table,
    held,
    depths,
    owner,
    level,
    slot_row,
    slot_at,
    want_row,
    wants,
    wants_at,
    packed,
    got,
    chosen,
    pixels,
    phase,
    spectrum,
    intensity,
    ring_sem,
    local_sem,
    row_send,
    row_recv,
    want_send,
    want_recv,
    pack_send,
    pack_recv,
    pixel_send,
    pixel_recv,
    phase_send,
    phase_recv,
    out_send,
    out_recv,
):
    count, rows, extent = patches.shape
    spread = extent // rows
    ring = spread // 2
    own = count // spread
    side = math.isqrt(tiles)
    me_t, me_d = lax.axis_index("tile"), lax.axis_index("depth")
    me_y, me_x, me_z, me_c = me_t // side, me_t % side, me_d // 2, me_d % 2

    def peer(step):
        hop, swap = near_first(step // 2), step % 2
        to = ((me_z + ring + hop) % ring) * 2 + (me_c + swap) % 2
        source = ((me_z + ring - hop) % ring) * 2 + (me_c + swap) % 2
        return to, source

    def shifted(down, over):
        to = ((me_y + down) % side) * side + (me_x + over) % side
        source = ((me_y + side - down) % side) * side + (me_x + side - over) % side
        return to, source

    reach, ring_rounds = reaches(spread)

    def within(distance):
        return min(2 * (2 * distance + 1), spread)

    barrier = pltpu.get_barrier_semaphore()

    @pl.loop(1, within(reach))
    def _(step):
        pl.semaphore_signal(barrier, inc=1, device_id={"depth": peer(within(reach) - step)[0]})

    @pl.loop(1, side)
    def _(shift):
        pl.semaphore_signal(barrier, inc=1, device_id={"tile": shifted(0, shift)[0]})
        pl.semaphore_signal(barrier, inc=1, device_id={"tile": shifted(shift, 0)[0]})

    def tell_ring(turn):
        for way, hop in enumerate((reach, ring - reach)):
            to = ((me_z + hop) % ring) * 2 + me_c
            pl.semaphore_signal(ring_sem.at[turn, way], inc=1, device_id={"depth": to})

    def learn_ring(turn):
        for way in range(2):
            pl.semaphore_wait(ring_sem.at[turn, way], 1)
        if turn + 1 < ring_rounds:
            tell_ring(turn + 1)
        send_pixels(turn + 1)

    load_owner = pltpu.make_async_copy(owners_in, owner, local_sem.at[3])
    load_owner.start()
    load_level = pltpu.make_async_copy(levels_in, level, local_sem.at[4 + own])
    load_level.start()
    load_held = pltpu.make_async_copy(patches, held, local_sem.at[5 + own])
    load_held.start()
    load_depths = pltpu.make_async_copy(phases, depths, local_sem.at[0])
    load_depths.start()
    load_table = pltpu.make_async_copy(tables, table, local_sem.at[1])
    load_table.start()
    load_pixels = pltpu.make_async_copy(
        patches.at[pl.ds(me_d * own, own)], pixels.at[:, pl.ds(me_d * rows, rows), :], local_sem.at[2]
    )
    load_pixels.start()

    load_owner.wait()
    load_level.wait()

    lane = lax.broadcasted_iota(jnp.int32, (1, LANES), 1)
    owners = lax.fori_loop(
        0, count, lambda p, row: jnp.where(lane == p, owner[0, p], row), jnp.full((1, LANES), -1, jnp.int32)
    )
    ranks = lax.fori_loop(
        0,
        count,
        lambda p, row: row + jnp.where((owners == owner[0, p]) & (lane > p), 1, 0),
        jnp.zeros((1, LANES), jnp.int32),
    )
    slot_row[...] = owners * CAP + ranks
    load_slots = pltpu.make_async_copy(slot_row, slot_at, local_sem.at[3])
    load_slots.start()
    load_slots.wait()
    wanted = lax.fori_loop(
        0,
        count,
        lambda p, row: jnp.where(lane == slot_at[0, p], level[0, p], row),
        jnp.zeros((1, LANES), jnp.int32),
    )
    want_row[...] = wanted
    wants[me_t] = wanted

    pl.semaphore_wait(barrier, within(reach) - 1 + 2 * (side - 1))
    tell_ring(0)

    def row_copy(shift, source):
        return pltpu.make_async_remote_copy(
            src_ref=want_row,
            dst_ref=wants.at[source],
            send_sem=row_send.at[shift],
            recv_sem=row_recv.at[shift],
            device_id={"tile": shifted(0, shift)[0]},
        )

    def want_copy(shift, source_row):
        return pltpu.make_async_remote_copy(
            src_ref=wants.at[pl.ds(me_y * side, side)],
            dst_ref=wants.at[pl.ds(source_row * side, side)],
            send_sem=want_send.at[shift],
            recv_sem=want_recv.at[shift],
            device_id={"tile": shifted(shift, 0)[0]},
        )

    def pixel_copy(step, to, source):
        return pltpu.make_async_remote_copy(
            src_ref=held.at[pl.ds(to * own, own)],
            dst_ref=pixels.at[:, pl.ds(source * rows, rows), :],
            send_sem=pixel_send.at[step],
            recv_sem=pixel_recv.at[step],
            device_id={"depth": to},
        )

    def pack_copy(step, to, source):
        return pltpu.make_async_remote_copy(
            src_ref=packed.at[to],
            dst_ref=got.at[pl.ds(source * CAP, CAP)],
            send_sem=pack_send.at[step],
            recv_sem=pack_recv.at[step],
            device_id={"tile": to},
        )

    def phase_copy(which, step, to, source):
        return pltpu.make_async_remote_copy(
            src_ref=chosen.at[which, to],
            dst_ref=phase.at[which, pl.ds(source * rows, rows), :],
            send_sem=phase_send.at[which, step],
            recv_sem=phase_recv.at[which, step],
            device_id={"depth": to},
        )

    def out_copy(which, step, to, source):
        return pltpu.make_async_remote_copy(
            src_ref=intensity.at[which, pl.ds(to * rows, rows), :],
            dst_ref=out.at[source * own + which],
            send_sem=out_send.at[which, step],
            recv_sem=out_recv.at[which, step],
            device_id={"depth": to},
        )

    def send_pixels(turn):
        first = 1 if turn == 0 else within(turn * reach)

        @pl.loop(first, within((turn + 1) * reach))
        def _(step):
            pixel_copy(step, peer(step)[0], me_d).start()

    def send_packed(down, over):
        to = shifted(down, over)[0]
        for slot in range(CAP):
            packed[to, slot] = depths[wants_at[to, 0, me_t * CAP + slot]]
        pack_copy(down * side + over, to, me_t).start()

    def read_wants(row):
        load = pltpu.make_async_copy(
            wants.at[pl.ds(row * side, side)], wants_at.at[pl.ds(row * side, side)], local_sem.at[3]
        )
        load.start()
        load.wait()

    @pl.loop(1, side)
    def _(shift):
        row_copy(shift, me_t).start()

    load_held.wait()
    send_pixels(0)
    learn_ring(0)

    @pl.loop(1, side)
    def _(shift):
        row_copy(shift, shifted(0, shift)[1]).wait_recv()

    @pl.loop(1, side)
    def _(shift):
        want_copy(shift, me_y).start()

    for turn in range(1, ring_rounds):
        learn_ring(turn)
    load_depths.wait()
    read_wants(me_y)

    @pl.loop(1, side)
    def _(over):
        send_packed(0, over)

    @pl.loop(1, side)
    def _(turn):
        down = (side + near_first(turn)) % side
        want_copy(side - down, (me_y + down) % side).wait_recv()
        read_wants((me_y + down) % side)

        @pl.loop(0, side)
        def _(over):
            send_packed(down, over)

    for slot in range(CAP):
        got[me_t * CAP + slot] = depths[wants_at[me_t, 0, me_t * CAP + slot]]

    @pl.loop(1, tiles)
    def _(step):
        to, source = shifted(step // side, step % side)
        pack_copy(step, to, source).wait_recv()

    @pl.loop(0, own)
    def _(which):
        @pl.loop(1, spread)
        def _(turn):
            step = spread - turn
            to = peer(step)[0]
            chosen[which, to] = got[slot_at[0, to * own + which]]
            phase_copy(which, step, to, me_d).start()

        phase[which, pl.ds(me_d * rows, rows), :] = got[slot_at[0, me_d * own + which]]

    load_table.wait()
    load_pixels.wait()

    @pl.loop(1, spread)
    def _(step):
        to, source = peer(step)
        pixel_copy(step, to, source).wait_recv()

    @pl.loop(0, own)
    def _(which):
        columns = apply_left(table[...], pixels[which])
        both = apply_left_transposed(table[...], columns)
        spectrum[which, 0] = both[:extent, :extent] - both[extent:, extent:]
        spectrum[which, 1] = -(both[:extent, extent:] + both[extent:, :extent])

    @pl.loop(0, own)
    def _(which):
        @pl.loop(1, spread)
        def _(step):
            to, source = peer(step)
            phase_copy(which, step, to, source).wait_recv()

        cosine, sine = cos_sin(phase[which])
        scale = 1.0 / float(extent * extent)
        real, imag = spectrum[which, 0] * scale, spectrum[which, 1] * scale
        moved = jnp.concatenate([real * cosine - imag * sine, real * sine + imag * cosine], axis=1)
        both = apply_left(table[...], moved)
        back = jnp.concatenate(
            [both[:extent, :extent] - both[extent:, extent:], both[:extent, extent:] + both[extent:, :extent]], axis=0
        )
        both = apply_left_transposed(table[...], back)
        field_real = both[:extent, :extent] - both[extent:, extent:]
        field_imag = both[:extent, extent:] + both[extent:, :extent]
        intensity[which] = field_real * field_real + field_imag * field_imag

        @pl.when(which < own - 1)
        def _():
            @pl.loop(1, spread)
            def _(turn):
                step = spread - turn
                out_copy(which, step, peer(step)[0], me_d).start()

        @pl.when(which == own - 1)
        def _():
            for low, high in zip(EDGES, EDGES[1:]):

                @pl.loop(1, spread)
                def _(turn):
                    step = spread - turn
                    to = peer(step)[0]

                    @pl.when((to * 8 >= low * spread) & (to * 8 < high * spread))
                    def _():
                        out_copy(which, step, to, me_d).start()

        pltpu.make_async_copy(
            intensity.at[which, pl.ds(me_d * rows, rows), :], out.at[me_d * own + which], local_sem.at[4 + which]
        ).start()

    @pl.loop(1, side)
    def _(shift):
        row_copy(shift, me_t).wait_send()
        want_copy(shift, me_y).wait_send()

    @pl.loop(1, tiles)
    def _(step):
        to, source = shifted(step // side, step % side)
        pack_copy(step, to, source).wait_send()

    @pl.loop(1, spread)
    def _(step):
        to, source = peer(step)
        pixel_copy(step, to, source).wait_send()

    @pl.loop(0, own)
    def _(which):
        @pl.loop(1, spread)
        def _(step):
            to, source = peer(step)
            phase_copy(which, step, to, source).wait_send()
            out_copy(which, step, to, source).wait()

        pltpu.make_async_copy(
            intensity.at[which, pl.ds(me_d * rows, rows), :], out.at[me_d * own + which], local_sem.at[4 + which]
        ).wait()


def solution(mesh):
    tiles, spread = mesh.shape["tile"], mesh.shape["depth"]

    def on_device(patches, patch_owner, patch_level, phases):
        count, rows, extent = patches.shape
        own = count // spread
        depth_count = phases.shape[0]
        ring_rounds, side = reaches(spread)[1], math.isqrt(tiles)
        tables = jnp.asarray(dft_tables(extent))
        any_space = pl.BlockSpec(memory_space=pl.ANY)
        f32, dma = jnp.float32, pltpu.SemaphoreType.DMA
        return pl.pallas_call(
            functools.partial(kernel, tiles),
            out_shape=pltpu.VMEM(patches.shape, patches.dtype),
            in_specs=[any_space] * 5,
            out_specs=pl.BlockSpec(memory_space=pltpu.VMEM),
            scratch_shapes=[
                pltpu.VMEM(tables.shape, tables.dtype),
                pltpu.VMEM(patches.shape, f32),
                pltpu.VMEM((depth_count, rows, extent), f32),
                pltpu.SMEM((1, count), jnp.int32),
                pltpu.SMEM((1, count), jnp.int32),
                pltpu.VMEM((1, LANES), jnp.int32),
                pltpu.SMEM((1, LANES), jnp.int32),
                pltpu.VMEM((1, LANES), jnp.int32),
                pltpu.VMEM((tiles, 1, LANES), jnp.int32),
                pltpu.SMEM((tiles, 1, LANES), jnp.int32),
                pltpu.VMEM((tiles, CAP, rows, extent), f32),
                pltpu.VMEM((tiles * CAP, rows, extent), f32),
                pltpu.VMEM((own, spread, rows, extent), f32),
                pltpu.VMEM((own, extent, extent), f32),
                pltpu.VMEM((own, extent, extent), f32),
                pltpu.VMEM((own, 2, extent, extent), f32),
                pltpu.VMEM((own, extent, extent), f32),
                pltpu.SemaphoreType.REGULAR((ring_rounds, 2)),
                dma((6 + own,)),
                dma((side,)),
                dma((side,)),
                dma((side,)),
                dma((side,)),
                dma((tiles,)),
                dma((tiles,)),
                dma((spread,)),
                dma((spread,)),
                dma((own, spread)),
                dma((own, spread)),
                dma((own, spread)),
                dma((own, spread)),
            ],
            compiler_params=pltpu.CompilerParams(
                collective_id=0, has_side_effects=True, vmem_limit_bytes=60 * 1024 * 1024
            ),
        )(
            patches,
            patch_owner.reshape(1, count),
            patch_level.reshape(1, count),
            jnp.transpose(phases, (0, 2, 1)),
            tables,
        )

    return jax.shard_map(
        on_device,
        mesh=mesh,
        in_specs=(P("tile", "depth", None), P("tile", None), P("tile"), P("tile", None, "depth")),
        out_specs=P("tile", "depth", None),
        check_vma=False,
    )
```
